32 devices in a mesh: dp: 8 (over y, x, core), tensor: 4 (over z).
Axes of the slice: x: 2, y: 2, z: 4, core: 2. Of those that a mesh axis runs over, the one named last changes fastest.
Arguments:
- queries: bfloat16 [128, 128, 8192], P('dp', None, 'tensor'), may hold values from -6 to 6
- block_kv: bfloat16 [128, 128, 2048], P('dp', None, 'tensor'), may hold values from -6 to 6
- cache: bfloat16 [16, 1024, 2048], P('dp', None, 'tensor'), may hold values from -6 to 6
- cache_len: int32 [16], P('dp'), may hold values from 2 to 1024
- block_counts: int32 [16], P('dp'), may hold values from 0 to 8
- destination: int32 [128], P('dp'), may hold values from -1 to 159, as said below
- branch: int32 [128, 128], P('dp'), may hold values from 0 to 3
- gain: float32 [8192], P('tensor'), may hold values from 0.1 to 1.9
Outputs:
- attended: bfloat16 [160, 128, 8192], P('dp', None, 'tensor')
The draws below stay inside these ranges and needn't reach their ends.
Inputs may be any that keep to these rules, and one draw needn't show every extreme that they name: `destination`: live blocks have distinct places; dead blocks have -1. A block whose place lies on another index of dp goes to the index d places after its own (the last index followed by the first), with d one of 1 to 3 or 8 // 2, at most one block of a device for each d.
All inputs are finite; a program needn't handle non-finite values.
Results may differ from the reference program's by a relative error of at most 0.0049.
Values may be sent and summed in bfloat16 or wider, within the bound.
A program may use at most 192 MiB of HBM per device.

```python
import jax
import jax.numpy as jnp
from jax import lax

HEADS = 64
KVH = 8
HD = 128
BLK = 128
BLK_MAX = 8
MOVE = 4
CACHE = 1024
SEQ_DEV = 2
SEQS = 16
SLOTS = 16
OUT_SLOTS = 20
N_DP = 8


def draw_plan(key):
    base_key = jax.random.fold_in(key, 4242)
    key_cap, key_count, key_offset = jax.random.split(base_key, 3)
    dev_caps = jax.random.randint(key_cap, (N_DP,), 1, BLK_MAX + 1)
    drawn = jax.random.randint(key_count, (N_DP, SEQ_DEV), 0, BLK_MAX + 1)
    counts = (drawn * dev_caps[:, None] + BLK_MAX - 1) // BLK_MAX
    counts = counts.at[0].set(BLK_MAX).astype(jnp.int32)
    slot_ids = jnp.arange(SLOTS, dtype=jnp.int32)
    is_live = (slot_ids % BLK_MAX)[None, :] < jnp.repeat(counts, BLK_MAX, axis=1)
    rank_ids = jnp.cumsum(is_live.astype(jnp.int32), axis=1) - 1
    excess = rank_ids - SLOTS // 2
    moving = is_live & (excess >= 0) & (excess < MOVE)
    distances = jnp.concatenate([jnp.arange(1, MOVE, dtype=jnp.int32), jnp.array([N_DP // 2], jnp.int32)])
    order = jax.random.permutation(key_offset, MOVE).astype(jnp.int32)
    offsets = distances[order]
    dev_ids = jnp.arange(N_DP, dtype=jnp.int32)[:, None]
    move_rank = jnp.clip(excess, 0, MOVE - 1)
    away_slot = (dev_ids + offsets[move_rank]) % N_DP * OUT_SLOTS + SLOTS + move_rank
    home_slot = dev_ids * OUT_SLOTS + slot_ids[None, :]
    dest_ids = jnp.where(moving, away_slot, jnp.where(is_live, home_slot, -1))
    return (counts.reshape(-1).astype(jnp.int32), dest_ids.reshape(-1).astype(jnp.int32))


def draw_block_counts(key, part):
    return draw_plan(key)[0]


def draw_destination(key, part):
    return draw_plan(key)[1]


def draw_queries(key, part):
    key_base = jax.random.fold_in(jax.random.fold_in(key, 1111), 0)
    shape = (SEQS * BLK_MAX, BLK, HEADS * HD)
    values = jnp.clip(jax.random.normal(key_base, shape, jnp.float32), -6.0, 6.0)
    return values.astype(jnp.bfloat16)


def draw_cache(key, part):
    key_base = jax.random.fold_in(key, 2222)
    shape = (SEQS, CACHE, KVH * 2 * HD)
    values = jnp.clip(jax.random.normal(key_base, shape, jnp.float32), -6.0, 6.0)
    return values.astype(jnp.bfloat16)


def with_ends(entries, stream_key, low, high):
    spot = [jax.random.randint(jax.random.fold_in(stream_key, axis), (), 0, length) for axis, length in enumerate(entries.shape)]
    main_axis = entries.shape.index(max(entries.shape))
    neighbour = spot[:main_axis] + [(spot[main_axis] + 1) % entries.shape[main_axis]] + spot[main_axis + 1:]
    return entries.at[tuple(spot)].set(low).at[tuple(neighbour)].set(high)


def block_scale(stream_key, shape, pieces, low, largest):
    def one(dim, parts):
        draws = jax.random.uniform(jax.random.fold_in(jax.random.fold_in(stream_key, 6), dim), (parts,), jnp.float32, low / len(pieces), largest / len(pieces))
        return jnp.repeat(jnp.exp(draws), shape[dim] // parts).reshape((-1,) + (1,) * (len(shape) - dim - 1))

    level = one(*pieces[0])
    for cut in pieces[1:]:
        level = level * one(*cut)
    return level


def bell_draw(key, dims, deviation, reach, cuts=(), kind=jnp.bfloat16):
    level = block_scale(key, dims, cuts, -0.22, 0.18) if cuts else 1.0
    values = jax.random.normal(key, dims, jnp.float32) * deviation * level
    return jnp.minimum(jnp.maximum(values, -reach), reach).astype(kind)


def setup_inputs(seed: int = 0) -> dict:
    key_list = jax.random.split(jax.random.key(seed), 9)
    return {
        "queries": draw_queries(jax.random.fold_in(key_list[8], 71), 0),
        "block_kv": bell_draw(key_list[1], (SEQS * BLK_MAX, BLK, KVH * 2 * HD), 1.0, 6.0, ((0, 8), (2, 4))),
        "cache": draw_cache(jax.random.fold_in(key_list[8], 71), 0),
        "cache_len": with_ends(jax.random.randint(key_list[3], (SEQS,), 2, CACHE + 1), jax.random.fold_in(key_list[3], 1), 2, CACHE).astype(jnp.int32),
        "block_counts": draw_block_counts(jax.random.fold_in(key_list[8], 71), 0),
        "destination": draw_destination(jax.random.fold_in(key_list[8], 71), 0),
        "branch": with_ends(jax.random.randint(key_list[6], (SEQS * BLK_MAX, BLK), 0, 4), jax.random.fold_in(key_list[6], 1), 0, 3).astype(jnp.int32),
        "gain": jnp.clip(1.0 + 0.18 * jax.random.normal(key_list[7], (HEADS * HD,), jnp.float32), 0.1, 1.9),
    }


epsilon = 1e-05

def attend(query, block_kv, cache, length, branch):
    row_count = query.shape[0]
    n_cache = cache.shape[0]
    joined_kv = jnp.concatenate([cache, block_kv], 0)
    kv_heads = joined_kv.shape[1] // (2 * HD)
    group_size = query.shape[1] // (HD * kv_heads)
    kv_pairs = joined_kv.reshape(joined_kv.shape[0], kv_heads, 2, HD).astype(jnp.float32)
    key_rows = kv_pairs[:, :, 0]
    value_rows = kv_pairs[:, :, 1]
    grouped = query.reshape(row_count, kv_heads, group_size, HD).astype(jnp.float32)
    scores = jnp.einsum('tkgd,nkd->kgtn', grouped, key_rows) * HD ** (-0.5)
    cache_pos = jnp.arange(n_cache, dtype=jnp.int32)
    cache_allowed = jnp.broadcast_to((cache_pos < length)[None, :], (row_count, n_cache))
    token_ids = jnp.arange(row_count, dtype=jnp.int32)
    block_allowed = (token_ids[None, :] <= token_ids[:, None]) & (branch[None, :] == branch[:, None])
    allowed = jnp.concatenate([cache_allowed, block_allowed], 1)
    scores = jnp.where(allowed[None, None], scores, jnp.float32(-1e+30))
    row_max = lax.optimization_barrier(jnp.max(scores, axis=-1, keepdims=True))
    shifted = jnp.exp(scores - row_max)
    probs = shifted / lax.optimization_barrier(jnp.sum(shifted, axis=-1, keepdims=True))
    weights = lax.optimization_barrier(probs.astype(jnp.bfloat16)).astype(jnp.float32)
    result = jnp.einsum('kgtn,nkd->tkgd', weights, value_rows)
    return result.reshape(row_count, -1)

def reference(queries, block_kv, cache, cache_len, block_counts, destination, branch, gain):
    total_blocks = queries.shape[0]

    def one_block(block_id):
        seq_id = block_id // BLK_MAX
        result = attend(queries[block_id], block_kv[block_id], cache[seq_id], cache_len[seq_id], branch[block_id])
        row_sums = lax.optimization_barrier(jnp.sum(result * result, axis=1, keepdims=True))
        return (result * lax.rsqrt(row_sums / (HEADS * HD) + epsilon) * gain).astype(jnp.bfloat16)
    block_ids = jnp.arange(total_blocks, dtype=jnp.int32)
    finished = lax.map(one_block, block_ids)
    is_live = block_ids % BLK_MAX < block_counts[block_ids // BLK_MAX]
    slot_ids = jnp.where(is_live, destination, N_DP * OUT_SLOTS).astype(jnp.int32)
    empty = jnp.zeros((N_DP * OUT_SLOTS, queries.shape[1], queries.shape[2]), jnp.bfloat16)
    return empty.at[slot_ids].set(finished, mode='drop')
```

```python
import functools
import math

import jax
import jax.numpy as jnp
from jax import lax
from jax.experimental import pallas as pl
from jax.experimental.pallas import tpu as pltpu
from jax.sharding import PartitionSpec as P

HEADS = 64
KVH = 8
HD = 128
BLK_MAX = 8
MOVE = 4
EPS = 1e-05
SCALE = math.log2(math.e) / math.sqrt(HD)
SAFE = 60.0 * math.log2(math.e)
CHUNK = 256
ROWS = 512
VMEM_LIMIT = 48 * 1024 * 1024


def scores_of(q, k):
    return lax.dot_general(q, k, (((1,), (1,)), ((), ())), preferred_element_type=jnp.float32)


def attend_kernel(slot_ref, seq_ref, live_ref, fresh_ref, len_ref,
                  q_ref, bkv_ref, cache_ref, branch_ref,
                  out_ref, sums_ref, vaug, qrows, acc, rowmax, norm_ref):
    step = pl.program_id(0)
    n_cache, kv_cols = cache_ref.shape[1], cache_ref.shape[2]
    heads_kv = kv_cols // (2 * HD)
    toks = q_ref.shape[1]
    group = q_ref.shape[2] // (HD * heads_kv)
    rows = group * toks

    @pl.when(fresh_ref[step] == 1)
    def _():
        length = len_ref[seq_ref[step]]
        pos = lax.broadcasted_iota(jnp.int32, (n_cache, HD), 0)
        seen = pos < length
        best = jnp.zeros((n_cache, 1), jnp.float32)
        for g in range(heads_kv):
            key = cache_ref[0, :, g * 2 * HD:g * 2 * HD + HD].astype(jnp.float32)
            val = cache_ref[0, :, g * 2 * HD + HD:(g + 1) * 2 * HD].astype(jnp.float32)
            vaug[g, :, :HD] = jnp.where(seen, val, 0.0).astype(jnp.bfloat16)
            vaug[g, :, HD:] = jnp.where(seen, 1.0, 0.0).astype(jnp.bfloat16)
            best = jnp.maximum(best, jnp.sum(key * key, axis=1, keepdims=True))
        norm_ref[0] = jnp.max(best)

    @pl.when(live_ref[step] == 1)
    def _():
        length = len_ref[seq_ref[step]]
        chunks = (length + CHUNK - 1) // CHUNK
        qbest = jnp.zeros((toks, 1), jnp.float32)
        kbest = jnp.zeros((toks, 1), jnp.float32)
        for g in range(heads_kv):
            for h in range(group):
                head = g * group + h
                slab = q_ref[0, :, head * HD:(head + 1) * HD]
                qrows[g, h * toks:(h + 1) * toks, :] = slab
                wide = slab.astype(jnp.float32)
                qbest = jnp.maximum(qbest, jnp.sum(wide * wide, axis=1, keepdims=True))
            key = bkv_ref[0, :, g * 2 * HD:g * 2 * HD + HD].astype(jnp.float32)
            kbest = jnp.maximum(kbest, jnp.sum(key * key, axis=1, keepdims=True))
        knorm = jnp.maximum(norm_ref[0], jnp.max(kbest))
        qnorm = jnp.max(qbest)
        limit = SAFE / SCALE
        small = qnorm * knorm < limit * limit

        tags = jnp.broadcast_to(branch_ref[0].astype(jnp.float32), (toks, toks))
        older = lax.broadcasted_iota(jnp.int32, (toks, toks), 1) <= lax.broadcasted_iota(
            jnp.int32, (toks, toks), 0)
        allowed = older & (tags == tags.T)

        def parts():
            for g in range(heads_kv):
                for r in range(0, rows, ROWS):
                    yield g, r

        def block_key(g):
            return bkv_ref[0, :, g * 2 * HD:g * 2 * HD + HD]

        def block_value(g):
            val = bkv_ref[0, :, g * 2 * HD + HD:(g + 1) * 2 * HD]
            return jnp.concatenate([val, jnp.ones_like(val)], 1)

        def chunk_key(g, start):
            return cache_ref[0, pl.ds(start, CHUNK), g * 2 * HD:g * 2 * HD + HD]

        mask = jnp.concatenate([allowed] * (ROWS // toks), 0)

        def run(safe):
            def power(s, g, r):
                s = s * SCALE
                if safe:
                    s = jnp.minimum(s - rowmax[g, r:r + ROWS, :1], 0.0)
                return jnp.exp2(s)

            for g, r in parts():
                s = scores_of(qrows[g, r:r + ROWS, :], block_key(g))
                p = jnp.where(mask, power(s, g, r), 0.0).astype(jnp.bfloat16)
                acc[g, r:r + ROWS, :] = jnp.dot(
                    p, block_value(g), preferred_element_type=jnp.float32)

            def body(c, carry):
                start = pl.multiple_of(c * CHUNK, CHUNK)
                for g, r in parts():
                    s = scores_of(qrows[g, r:r + ROWS, :], chunk_key(g, start))
                    p = power(s, g, r).astype(jnp.bfloat16)
                    acc[g, r:r + ROWS, :] += jnp.dot(
                        p, vaug[g, pl.ds(start, CHUNK), :], preferred_element_type=jnp.float32)
                return carry

            lax.fori_loop(0, chunks, body, 0)

        @pl.when(small)
        def _():
            run(False)

        @pl.when(jnp.logical_not(small))
        def _():
            for g, r in parts():
                s = scores_of(qrows[g, r:r + ROWS, :], block_key(g)) * SCALE
                top = jnp.max(jnp.where(mask, s, -1e30), axis=1, keepdims=True)
                rowmax[g, r:r + ROWS, :] = jnp.broadcast_to(top, (ROWS, HD))

            def body(c, carry):
                start = pl.multiple_of(c * CHUNK, CHUNK)
                pos = start + lax.broadcasted_iota(jnp.int32, (ROWS, CHUNK), 1)
                for g, r in parts():
                    s = scores_of(qrows[g, r:r + ROWS, :], chunk_key(g, start)) * SCALE
                    top = jnp.max(jnp.where(pos < length, s, -1e30), axis=1, keepdims=True)
                    rowmax[g, r:r + ROWS, :] = jnp.maximum(
                        rowmax[g, r:r + ROWS, :], jnp.broadcast_to(top, (ROWS, HD)))
                return carry

            lax.fori_loop(0, chunks, body, 0)
            run(True)

        total = jnp.zeros((toks, HD), jnp.float32)
        for g in range(heads_kv):
            for h in range(group):
                head = g * group + h
                here = slice(h * toks, (h + 1) * toks)
                res = acc[g, here, :HD] / acc[g, here, HD:]
                total = total + res * res
                out_ref[0, :, head * HD:(head + 1) * HD] = res.astype(jnp.bfloat16)
        sums_ref[0] = jnp.sum(total.T, axis=0, keepdims=True)


def attend_blocks(slot, out_slot, live, out_count, queries, block_kv, cache, cache_len, branch):
    slots, toks, cols = queries.shape
    kv_cols = cache.shape[2]
    n_cache = cache.shape[1]
    heads_kv = kv_cols // (2 * HD)
    rows = cols // HD // heads_kv * toks
    steps = slot.shape[0]
    seq = slot // BLK_MAX
    same = jnp.concatenate([jnp.zeros((1,), jnp.int32), ((seq[1:] == seq[:-1]) & (live[:-1] == 1)).astype(jnp.int32)])
    fresh = live * (1 - same)
    keys = n_cache + toks
    return pl.pallas_call(
        attend_kernel,
        grid_spec=pltpu.PrefetchScalarGridSpec(
            num_scalar_prefetch=6,
            grid=(steps,),
            in_specs=[
                pl.BlockSpec((1, toks, cols), lambda i, o, s, *_: (s[i], 0, 0)),
                pl.BlockSpec((1, toks, kv_cols), lambda i, o, s, *_: (s[i], 0, 0)),
                pl.BlockSpec((1, n_cache, kv_cols), lambda i, o, s, q, *_: (q[i], 0, 0)),
                pl.BlockSpec((1, 1, toks), lambda i, o, s, *_: (s[i], 0, 0)),
            ],
            out_specs=[
                pl.BlockSpec((1, toks, cols), lambda i, o, *_: (o[i], 0, 0)),
                pl.BlockSpec((1, 1, toks), lambda i, o, *_: (o[i], 0, 0)),
            ],
            scratch_shapes=[
                pltpu.VMEM((heads_kv, n_cache, 2 * HD), jnp.bfloat16),
                pltpu.VMEM((heads_kv, rows, HD), jnp.bfloat16),
                pltpu.VMEM((heads_kv, rows, 2 * HD), jnp.float32),
                pltpu.VMEM((heads_kv, rows, HD), jnp.float32),
                pltpu.SMEM((1,), jnp.float32),
            ],
        ),
        out_shape=[
            jax.ShapeDtypeStruct((out_count, toks, cols), jnp.bfloat16),
            jax.ShapeDtypeStruct((out_count, 1, toks), jnp.float32),
        ],
        compiler_params=pltpu.CompilerParams(
            dimension_semantics=("arbitrary",), vmem_limit_bytes=VMEM_LIMIT),
        cost_estimate=pl.CostEstimate(
            flops=steps * 4 * toks * cols * keys, transcendentals=steps * toks * keys * cols // HD,
            bytes_accessed=steps * toks * cols * 4),
    )(out_slot, slot, seq, live, fresh, cache_len, queries, block_kv, cache,
      branch.reshape(slots, 1, toks))


def drop_first(kernel):
    def inner(_, *refs):
        kernel(*refs)

    return inner


attend_kernel = drop_first(attend_kernel)


def place_kernel(count, kind_ref, home_ref, way_ref, ready_ref, sums_ref, far_sums_ref, gain_ref, *rest):
    parcels, out_ref = rest[:count], rest[count]
    step = pl.program_id(0)
    kind = kind_ref[step]
    toks = out_ref.shape[1]

    def emit(raw_ref, row):
        factor = lax.rsqrt(row / (HEADS * HD) + EPS)
        spread = jnp.broadcast_to(factor, (toks, toks)).T
        for col in range(0, out_ref.shape[2], HD):
            part = raw_ref[0, :, col:col + HD].astype(jnp.float32)
            out_ref[0, :, col:col + HD] = (
                part * spread * gain_ref[:, col:col + HD]).astype(jnp.bfloat16)

    @pl.when(kind == 0)
    def _():
        out_ref[...] = jnp.zeros_like(out_ref)

    @pl.when(kind == 1)
    def _():
        emit(ready_ref, sums_ref[home_ref[step]])

    for way in range(count):
        @pl.when((kind == 2) & (way_ref[step] == way))
        def _():
            emit(parcels[way], far_sums_ref[way])


def on_device(groups, queries, block_kv, cache, cache_len, block_counts, destination, branch, gain):
    slots, toks, cols = queries.shape
    out_slots = slots + MOVE
    me = lax.axis_index("dp")
    ways = sorted({d % groups for d in (1, 2, 3, groups // 2)} - {0})
    count = len(ways)
    slot_ids = jnp.arange(slots, dtype=jnp.int32)
    seq_of = slot_ids // BLK_MAX
    is_live = slot_ids % BLK_MAX < block_counts[seq_of]
    target_dev = destination // out_slots
    target_slot = destination % out_slots
    staying = is_live & (target_dev == me)
    leaving = is_live & (target_dev != me)

    peers = (me + jnp.array(ways, jnp.int32)) % groups
    matches = leaving[None, :] & (target_dev[None, :] == peers[:, None])
    moving = jnp.any(matches, axis=1)
    move_slot = jnp.sum(jnp.where(matches, slot_ids[None, :], 0), axis=1)
    send_slot = jnp.where(moving, jnp.sum(jnp.where(matches, target_slot[None, :], 0), axis=1), out_slots)

    rank = jnp.cumsum(staying.astype(jnp.int32)) - 1
    stay_total = jnp.sum(staying.astype(jnp.int32))
    step_rank = jnp.minimum(slot_ids, jnp.maximum(stay_total - 1, 0))
    stay_slot = jnp.sum(
        jnp.where(staying[None, :] & (rank[None, :] == step_rank[:, None]), slot_ids[None, :], 0), axis=1)
    stay_live = (slot_ids < stay_total).astype(jnp.int32)

    table = lax.all_gather(send_slot, "dp")
    from_dev = (me - jnp.array(ways, jnp.int32)) % groups
    arrived_slot = table[from_dev, jnp.arange(count)]

    move_raw, move_sums = attend_blocks(
        move_slot, jnp.arange(count, dtype=jnp.int32), moving.astype(jnp.int32), count,
        queries, block_kv, cache, cache_len, branch)
    move_sums = lax.psum(move_sums, "tensor")
    parcels, far_sums = [], []
    for way, d in enumerate(ways):
        hop = [(i, (i + d) % groups) for i in range(groups)]
        parcels.append(lax.ppermute(move_raw[way:way + 1], "dp", hop))
        far_sums.append(lax.ppermute(move_sums[way:way + 1], "dp", hop))
    ready, sums = attend_blocks(
        stay_slot, stay_slot, stay_live, slots, queries, block_kv, cache, cache_len, branch)
    sums = lax.psum(sums, "tensor")

    places = jnp.arange(out_slots, dtype=jnp.int32)
    at_home = staying[None, :] & (target_slot[None, :] == places[:, None])
    from_far = arrived_slot[None, :] == places[:, None]
    kind = jnp.where(jnp.any(at_home, axis=1), 1, jnp.where(jnp.any(from_far, axis=1), 2, 0)).astype(jnp.int32)
    home = lax.cummax(jnp.sum(jnp.where(at_home, slot_ids[None, :], 0), axis=1).astype(jnp.int32))
    home = jnp.where(kind == 1, jnp.sum(jnp.where(at_home, slot_ids[None, :], 0), axis=1), home).astype(jnp.int32)
    way = jnp.sum(jnp.where(from_far, jnp.arange(count)[None, :], 0), axis=1).astype(jnp.int32)
    whole = lambda shape: pl.BlockSpec(shape, lambda i, *_: (0,) * len(shape))
    return pl.pallas_call(
        functools.partial(place_kernel, count),
        grid_spec=pltpu.PrefetchScalarGridSpec(
            num_scalar_prefetch=3,
            grid=(out_slots,),
            in_specs=[
                pl.BlockSpec((1, toks, cols), lambda i, k, h, w: (h[i], 0, 0)),
                whole((slots, 1, toks)),
                whole((count, 1, toks)),
                whole((1, cols)),
            ] + [whole((1, toks, cols))] * count,
            out_specs=pl.BlockSpec((1, toks, cols), lambda i, *_: (i, 0, 0)),
        ),
        out_shape=jax.ShapeDtypeStruct((out_slots, toks, cols), jnp.bfloat16),
        compiler_params=pltpu.CompilerParams(
            dimension_semantics=("arbitrary",), vmem_limit_bytes=VMEM_LIMIT),
    )(kind, home, way, ready, sums, jnp.concatenate(far_sums, 0), gain.reshape(1, cols), *parcels)


def solution(mesh):
    placed = (
        P("dp", None, "tensor"),
        P("dp", None, "tensor"),
        P("dp", None, "tensor"),
        P("dp"),
        P("dp"),
        P("dp"),
        P("dp", None),
        P("tensor"),
    )
    return jax.shard_map(
        functools.partial(on_device, mesh.shape["dp"]),
        mesh=mesh, in_specs=placed, out_specs=P("dp", None, "tensor"), check_vma=False
    )
```

```python
import functools
import math

import jax
import jax.numpy as jnp
from jax import lax
from jax.experimental import pallas as pl
from jax.experimental.pallas import tpu as pltpu
from jax.sharding import PartitionSpec as P

HEADS = 64
KVH = 8
HD = 128
BLK_MAX = 8
MOVE = 4
EPS = 1e-05
SCALE = math.log2(math.e) / math.sqrt(HD)
SAFE = 60.0 * math.log2(math.e)
CHUNK = 256
ROWS = 512
VMEM_LIMIT = 48 * 1024 * 1024


def scores_of(q, k):
    return lax.dot_general(q, k, (((1,), (1,)), ((), ())), preferred_element_type=jnp.float32)


def attend_kernel(base, steps, lens, tab_ref, q_ref, bkv_ref, cache_ref, branch_ref,
                  out_ref, sums_ref, vaug, qrows, acc, rowmax, norm_ref):
    step = pl.program_id(0)
    n_cache, kv_cols = cache_ref.shape[1], cache_ref.shape[2]
    heads_kv = kv_cols // (2 * HD)
    toks = q_ref.shape[1]
    group = q_ref.shape[2] // (HD * heads_kv)
    rows = group * toks

    @pl.when(tab_ref[base + 3 * steps + step] == 1)
    def _():
        length = tab_ref[lens + tab_ref[base + steps + step]]
        pos = lax.broadcasted_iota(jnp.int32, (n_cache, HD), 0)
        seen = pos < length
        best = jnp.zeros((n_cache, 1), jnp.float32)
        for g in range(heads_kv):
            key = cache_ref[0, :, g * 2 * HD:g * 2 * HD + HD].astype(jnp.float32)
            val = cache_ref[0, :, g * 2 * HD + HD:(g + 1) * 2 * HD].astype(jnp.float32)
            vaug[g, :, :HD] = jnp.where(seen, val, 0.0).astype(jnp.bfloat16)
            vaug[g, :, HD:] = jnp.where(seen, 1.0, 0.0).astype(jnp.bfloat16)
            best = jnp.maximum(best, jnp.sum(key * key, axis=1, keepdims=True))
        norm_ref[0] = jnp.max(best)

    @pl.when(tab_ref[base + 2 * steps + step] == 1)
    def _():
        length = tab_ref[lens + tab_ref[base + steps + step]]
        chunks = (length + CHUNK - 1) // CHUNK
        qbest = jnp.zeros((toks, 1), jnp.float32)
        kbest = jnp.zeros((toks, 1), jnp.float32)
        for g in range(heads_kv):
            for h in range(group):
                head = g * group + h
                slab = q_ref[0, :, head * HD:(head + 1) * HD]
                qrows[g, h * toks:(h + 1) * toks, :] = slab
                wide = slab.astype(jnp.float32)
                qbest = jnp.maximum(qbest, jnp.sum(wide * wide, axis=1, keepdims=True))
            key = bkv_ref[0, :, g * 2 * HD:g * 2 * HD + HD].astype(jnp.float32)
            kbest = jnp.maximum(kbest, jnp.sum(key * key, axis=1, keepdims=True))
        knorm = jnp.maximum(norm_ref[0], jnp.max(kbest))
        qnorm = jnp.max(qbest)
        limit = SAFE / SCALE
        small = qnorm * knorm < limit * limit

        tags = jnp.broadcast_to(branch_ref[0].astype(jnp.float32), (toks, toks))
        older = lax.broadcasted_iota(jnp.int32, (toks, toks), 1) <= lax.broadcasted_iota(
            jnp.int32, (toks, toks), 0)
        allowed = older & (tags == tags.T)

        def parts():
            for g in range(heads_kv):
                for r in range(0, rows, ROWS):
                    yield g, r

        def block_key(g):
            return bkv_ref[0, :, g * 2 * HD:g * 2 * HD + HD]

        def block_value(g):
            val = bkv_ref[0, :, g * 2 * HD + HD:(g + 1) * 2 * HD]
            return jnp.concatenate([val, jnp.ones_like(val)], 1)

        def chunk_key(g, start):
            return cache_ref[0, pl.ds(start, CHUNK), g * 2 * HD:g * 2 * HD + HD]

        mask = jnp.concatenate([allowed] * (ROWS // toks), 0)

        def run(safe):
            def power(s, g, r):
                s = s * SCALE
                if safe:
                    s = jnp.minimum(s - rowmax[g, r:r + ROWS, :1], 0.0)
                return jnp.exp2(s)

            for g, r in parts():
                s = scores_of(qrows[g, r:r + ROWS, :], block_key(g))
                p = jnp.where(mask, power(s, g, r), 0.0).astype(jnp.bfloat16)
                acc[g, r:r + ROWS, :] = jnp.dot(
                    p, block_value(g), preferred_element_type=jnp.float32)

            def body(c, carry):
                start = pl.multiple_of(c * CHUNK, CHUNK)
                for g, r in parts():
                    s = scores_of(qrows[g, r:r + ROWS, :], chunk_key(g, start))
                    p = power(s, g, r).astype(jnp.bfloat16)
                    acc[g, r:r + ROWS, :] += jnp.dot(
                        p, vaug[g, pl.ds(start, CHUNK), :], preferred_element_type=jnp.float32)
                return carry

            lax.fori_loop(0, chunks, body, 0)

        @pl.when(small)
        def _():
            run(False)

        @pl.when(jnp.logical_not(small))
        def _():
            for g, r in parts():
                s = scores_of(qrows[g, r:r + ROWS, :], block_key(g)) * SCALE
                top = jnp.max(jnp.where(mask, s, -1e30), axis=1, keepdims=True)
                rowmax[g, r:r + ROWS, :] = jnp.broadcast_to(top, (ROWS, HD))

            def body(c, carry):
                start = pl.multiple_of(c * CHUNK, CHUNK)
                pos = start + lax.broadcasted_iota(jnp.int32, (ROWS, CHUNK), 1)
                for g, r in parts():
                    s = scores_of(qrows[g, r:r + ROWS, :], chunk_key(g, start)) * SCALE
                    top = jnp.max(jnp.where(pos < length, s, -1e30), axis=1, keepdims=True)
                    rowmax[g, r:r + ROWS, :] = jnp.maximum(
                        rowmax[g, r:r + ROWS, :], jnp.broadcast_to(top, (ROWS, HD)))
                return carry

            lax.fori_loop(0, chunks, body, 0)
            run(True)

        total = jnp.zeros((toks, HD), jnp.float32)
        for g in range(heads_kv):
            for h in range(group):
                head = g * group + h
                here = slice(h * toks, (h + 1) * toks)
                res = acc[g, here, :HD] / acc[g, here, HD:]
                total = total + res * res
                out_ref[0, :, head * HD:(head + 1) * HD] = res.astype(jnp.bfloat16)
        sums_ref[0] = jnp.sum(total.T, axis=0, keepdims=True)


def attend_blocks(tab, base, lens, steps, in_order, out_count, queries, block_kv, cache, branch):
    slots, toks, cols = queries.shape
    kv_cols = cache.shape[2]
    n_cache = cache.shape[1]
    heads_kv = kv_cols // (2 * HD)
    rows = cols // HD // heads_kv * toks
    keys = n_cache + toks

    def slot_map(i, t):
        return (t[base + i], 0, 0)

    def out_map(i, t):
        return (i, 0, 0) if in_order else (t[base + i], 0, 0)

    return pl.pallas_call(
        functools.partial(attend_kernel, base, steps, lens),
        grid_spec=pltpu.PrefetchScalarGridSpec(
            num_scalar_prefetch=1,
            grid=(steps,),
            in_specs=[
                pl.BlockSpec((1, toks, cols), slot_map),
                pl.BlockSpec((1, toks, kv_cols), slot_map),
                pl.BlockSpec((1, n_cache, kv_cols), lambda i, t: (t[base + steps + i], 0, 0)),
                pl.BlockSpec((1, 1, toks), slot_map),
            ],
            out_specs=[
                pl.BlockSpec((1, toks, cols), out_map),
                pl.BlockSpec((1, 1, toks), out_map),
            ],
            scratch_shapes=[
                pltpu.VMEM((heads_kv, n_cache, 2 * HD), jnp.bfloat16),
                pltpu.VMEM((heads_kv, rows, HD), jnp.bfloat16),
                pltpu.VMEM((heads_kv, rows, 2 * HD), jnp.float32),
                pltpu.VMEM((heads_kv, rows, HD), jnp.float32),
                pltpu.SMEM((1,), jnp.float32),
            ],
        ),
        out_shape=[
            jax.ShapeDtypeStruct((out_count, toks, cols), jnp.bfloat16),
            jax.ShapeDtypeStruct((out_count, 1, toks), jnp.float32),
        ],
        compiler_params=pltpu.CompilerParams(
            dimension_semantics=("arbitrary",), vmem_limit_bytes=VMEM_LIMIT),
        cost_estimate=pl.CostEstimate(
            flops=steps * 4 * toks * cols * keys, transcendentals=steps * toks * keys * cols // HD,
            bytes_accessed=steps * toks * cols * 4),
    )(tab, queries, block_kv, cache, branch.reshape(slots, 1, toks))


def plan_kernel(ways, groups, at, len_ref, count_ref, dest_ref, tab_ref):
    me = lax.axis_index("dp")
    slots = dest_ref.shape[0]
    out_slots = slots + MOVE
    count = len(ways)
    move, stay, home, send, lens = at["move"], at["stay"], at["home"], at["send"], at["lens"]
    for s in range(len_ref.shape[0]):
        tab_ref[lens + s] = len_ref[s]
    for o in range(out_slots):
        tab_ref[home + o] = jnp.int32(-1)
    for w in range(count):
        for field in range(4):
            tab_ref[move + field * count + w] = jnp.int32(0)
        tab_ref[send + w] = jnp.int32(out_slots)
    for i in range(slots):
        for field in range(4):
            tab_ref[stay + field * slots + i] = jnp.int32(0)

    def visit(i, total):
        seq = i // BLK_MAX
        place = jnp.maximum(dest_ref[i], 0)
        live = lax.rem(i, BLK_MAX) < count_ref[seq]
        dev = place // out_slots
        spot = lax.rem(place, out_slots)
        staying = live & (dev == me)

        @pl.when(staying)
        def _():
            tab_ref[stay + total] = i
            tab_ref[stay + slots + total] = seq
            tab_ref[stay + 2 * slots + total] = jnp.int32(1)
            tab_ref[home + spot] = i

        for w, d in enumerate(ways):
            peer = lax.rem(me + d, groups)

            @pl.when(live & (dev == peer))
            def _():
                tab_ref[move + w] = i
                tab_ref[move + count + w] = seq
                tab_ref[move + 2 * count + w] = jnp.int32(1)
                tab_ref[send + w] = spot

        return total + staying.astype(jnp.int32)

    total = lax.fori_loop(0, slots, visit, jnp.int32(0))
    last = jnp.maximum(total - 1, 0)

    def pad(i, carry):
        tab_ref[stay + i] = tab_ref[stay + last]
        tab_ref[stay + slots + i] = tab_ref[stay + slots + last]
        return carry

    lax.fori_loop(total, slots, pad, 0)

    def freshen(base, steps):
        def body(i, carry):
            before, loaded = carry
            seq = tab_ref[base + steps + i]
            live = tab_ref[base + 2 * steps + i]
            same = (seq == before) & (loaded == 1)
            tab_ref[base + 3 * steps + i] = jnp.where(same, 0, live)
            return jnp.where(live == 1, seq, before), jnp.maximum(live, loaded)

        lax.fori_loop(0, steps, body, (jnp.int32(0), jnp.int32(0)))

    freshen(move, count)
    freshen(stay, slots)


def exchange_kernel(ways, groups, peers, send_at, tab_ref, sums_ref, move_ref,
                    total_ref, far_ref, far_slot_ref,
                    got_sums, got_move, pay, land, send_sem, recv_sem, way_send, way_recv):
    me = lax.axis_index("dp")
    mine = lax.axis_index("tensor")
    for w in range(len(ways)):
        pay[w, 1:2, :] = jnp.full((1, pay.shape[2]), tab_ref[send_at + w].astype(jnp.float32))
    barrier = pltpu.get_barrier_semaphore()
    offsets = sorted({d for d in ways} | {groups - d for d in ways})
    for k in range(1, peers):
        pl.semaphore_signal(barrier, inc=1, device_id={"tensor": lax.rem(mine + k, peers)},
                            device_id_type=pl.DeviceIdType.MESH)
    for d in offsets:
        pl.semaphore_signal(barrier, inc=1, device_id={"dp": lax.rem(me + d, groups)},
                            device_id_type=pl.DeviceIdType.MESH)
    pl.semaphore_wait(barrier, peers - 1 + len(offsets))

    def remote(src, dst, send, recv, device):
        return pltpu.make_async_remote_copy(
            src_ref=src, dst_ref=dst, send_sem=send, recv_sem=recv, device_id=device,
            device_id_type=pl.DeviceIdType.MESH)

    near = []
    for k in range(1, peers):
        device = {"tensor": lax.rem(mine + k, peers)}
        near.append((
            remote(move_ref, got_move.at[k - 1], send_sem.at[2 * k - 2], recv_sem.at[2 * k - 2], device),
            remote(sums_ref, got_sums.at[k - 1], send_sem.at[2 * k - 1], recv_sem.at[2 * k - 1], device)))
    for first, _ in near:
        first.start()
    for _, second in near:
        second.start()
    total = move_ref[...]
    for k, (first, _) in enumerate(near):
        first.wait()
        total = total + got_move[k]
    pay[:, 0:1, :] = total
    whole = sums_ref[...]
    for k, (_, second) in enumerate(near):
        second.wait()
        whole = whole + got_sums[k]
    total_ref[...] = whole
    away = []
    for w, d in enumerate(ways):
        copy = remote(pay.at[w], land.at[w], way_send.at[w], way_recv.at[w], {"dp": lax.rem(me + d, groups)})
        copy.start()
        away.append(copy)
    for copy in away:
        copy.wait()
    far_ref[...] = land[:, 0:1, :]
    far_slot_ref[...] = land[:, 1:2, :]


def place_kernel(count, home_at, tab_ref, slot_ref, ready_ref, sums_ref, far_ref, gain_ref, *rest):
    parcels = rest[:count]
    out_ref, buf, blank, factors, in_sem, out_sem = rest[count:]
    out_slots, toks, cols = out_ref.shape
    slots = sums_ref.shape[0]
    factors[:slots] = lax.rsqrt(sums_ref[...] / (HEADS * HD) + EPS)
    factors[slots:] = lax.rsqrt(far_ref[...] / (HEADS * HD) + EPS)
    blank[...] = jnp.zeros_like(blank)

    def source(o):
        home = tab_ref[home_at + o]
        far = jnp.int32(-1)
        for w in range(count):
            far = jnp.where(slot_ref[w, 0, 0].astype(jnp.int32) == o, w, far)
        return home, far

    def fetch(o, carry):
        home, far = source(o)

        @pl.when(home >= 0)
        def _():
            pltpu.make_async_copy(ready_ref.at[home], buf.at[o], in_sem.at[o]).start()

        for w in range(count):
            @pl.when((home < 0) & (far == w))
            def _():
                pltpu.make_async_copy(parcels[w].at[0], buf.at[o], in_sem.at[o]).start()

        @pl.when((home < 0) & (far < 0))
        def _():
            pltpu.make_async_copy(blank, out_ref.at[o], out_sem.at[o]).start()

        return carry

    lax.fori_loop(0, out_slots, fetch, 0)

    def finish(o, carry):
        home, far = source(o)

        @pl.when((home >= 0) | (far >= 0))
        def _():
            pltpu.make_async_copy(ready_ref.at[0], buf.at[o], in_sem.at[o]).wait()
            row = jnp.where(home >= 0, home, slots + far)
            spread = jnp.broadcast_to(factors[row], (toks, toks)).T
            for col in range(0, cols, HD):
                part = buf[o, :, col:col + HD].astype(jnp.float32)
                buf[o, :, col:col + HD] = (
                    part * spread * gain_ref[:, col:col + HD]).astype(jnp.bfloat16)
            pltpu.make_async_copy(buf.at[o], out_ref.at[o], out_sem.at[o]).start()

        return carry

    lax.fori_loop(0, out_slots, finish, 0)

    def drain(o, carry):
        pltpu.make_async_copy(blank, out_ref.at[o], out_sem.at[o]).wait()
        return carry

    lax.fori_loop(0, out_slots, drain, 0)


def on_device(groups, tensor, queries, block_kv, cache, cache_len, block_counts, destination, branch, gain):
    slots, toks, cols = queries.shape
    out_slots = slots + MOVE
    ways = sorted({d % groups for d in (1, 2, 3, groups // 2)} - {0})
    count = len(ways)
    smem = pl.BlockSpec(memory_space=pltpu.SMEM)
    vmem = pl.BlockSpec(memory_space=pltpu.VMEM)
    hbm = pl.BlockSpec(memory_space=pl.ANY)
    at, size = {}, 0
    for name, length in (("move", 4 * count), ("stay", 4 * slots), ("home", out_slots),
                         ("send", count), ("lens", cache_len.shape[0])):
        at[name], size = size, size + length
    tab = pl.pallas_call(
        functools.partial(plan_kernel, ways, groups, at),
        in_specs=[smem] * 3, out_specs=smem,
        out_shape=jax.ShapeDtypeStruct((size,), jnp.int32),
    )(cache_len, block_counts, destination)

    move_raw, move_sums = attend_blocks(
        tab, at["move"], at["lens"], count, True, count, queries, block_kv, cache, branch)
    parcels = []
    for way, d in enumerate(ways):
        hop = [(i, (i + d) % groups) for i in range(groups)]
        parcels.append(lax.ppermute(move_raw[way:way + 1], "dp", hop))
    ready, sums = attend_blocks(
        tab, at["stay"], at["lens"], slots, False, slots, queries, block_kv, cache, branch)

    row = lambda n, rows=1: pltpu.VMEM((n, rows, toks), jnp.float32)
    sums, far_sums, far_slot = pl.pallas_call(
        functools.partial(exchange_kernel, ways, groups, tensor, at["send"]),
        in_specs=[smem, vmem, vmem], out_specs=[vmem] * 3,
        out_shape=[jax.ShapeDtypeStruct((n, 1, toks), jnp.float32) for n in (slots, count, count)],
        scratch_shapes=[
            pltpu.VMEM((tensor - 1, slots, 1, toks), jnp.float32),
            pltpu.VMEM((tensor - 1, count, 1, toks), jnp.float32),
            row(count, 2), row(count, 2),
            pltpu.SemaphoreType.DMA((2 * tensor - 2,)), pltpu.SemaphoreType.DMA((2 * tensor - 2,)),
            pltpu.SemaphoreType.DMA((count,)), pltpu.SemaphoreType.DMA((count,)),
        ],
        compiler_params=pltpu.CompilerParams(collective_id=0, has_side_effects=True),
    )(tab, sums, move_sums)

    return pl.pallas_call(
        functools.partial(place_kernel, count, at["home"]),
        in_specs=[smem, smem, hbm, vmem, vmem, vmem] + [hbm] * count,
        out_specs=hbm,
        out_shape=jax.ShapeDtypeStruct((out_slots, toks, cols), jnp.bfloat16),
        scratch_shapes=[
            pltpu.VMEM((out_slots, toks, cols), jnp.bfloat16),
            pltpu.VMEM((toks, cols), jnp.bfloat16),
            row(slots + count),
            pltpu.SemaphoreType.DMA((out_slots,)), pltpu.SemaphoreType.DMA((out_slots,)),
        ],
        compiler_params=pltpu.CompilerParams(vmem_limit_bytes=VMEM_LIMIT),
    )(tab, far_slot, ready, sums, far_sums, gain.reshape(1, cols), *parcels)


def solution(mesh):
    placed = (
        P("dp", None, "tensor"),
        P("dp", None, "tensor"),
        P("dp", None, "tensor"),
        P("dp"),
        P("dp"),
        P("dp"),
        P("dp", None),
        P("tensor"),
    )
    return jax.shard_map(
        functools.partial(on_device, mesh.shape["dp"], mesh.shape["tensor"]),
        mesh=mesh, in_specs=placed, out_specs=P("dp", None, "tensor"), check_vma=False
    )
```
